16 devices in a mesh: ep: 16 (over z, y, x, core).
Axes of the slice: x: 2, y: 2, z: 2, core: 2. Of those that a mesh axis runs over, the one named last changes fastest.
Arguments:
- tokens: bfloat16 [16384, 768], P('ep')
- grad_out: bfloat16 [16384, 768], P('ep')
- expert_ids: int32 [16384, 2], P('ep')
- w_gate: bfloat16 [768, 16], replicated
- w_in: bfloat16 [16, 768, 3072], P('ep')
- w_out: bfloat16 [16, 3072, 768], P('ep')
Outputs:
- output 1: bfloat16 [16384, 768], P('ep')
- output 2: bfloat16 [16384, 768], P('ep')
- output 3: float32 [16, 768, 3072], P('ep')
- output 4: float32 [16, 3072, 768], P('ep')
- output 5: float32 [768, 16], replicated
All inputs are finite; a program needn't handle non-finite values.
Results may differ from the reference program's by a relative error of at most 0.00483528.
Values are sent between devices in bfloat16 or wider.
A program may use at most 1 GiB of HBM per device.

```python
import jax
import jax.numpy as jnp
from jax import lax

EXPERTS = 16
TOKENS_DEV = 1024
D_MODEL = 768
D_HIDDEN = 3072
HOT_EXPERTS = 3

CAP_ROWS = TOKENS_DEV // 4
ALL_TOKENS = EXPERTS * TOKENS_DEV
CAP_ALL = EXPERTS * CAP_ROWS


def draw_routes(route_key):
    k_perm, k_shift, k_order, k_swap = jax.random.split(route_key, 4)
    n_cold = EXPERTS - HOT_EXPERTS
    cold_choices = 2 * TOKENS_DEV - HOT_EXPERTS * CAP_ROWS
    slot_pos = jnp.arange(2 * TOKENS_DEV)
    hot_rank = jnp.minimum(slot_pos // CAP_ROWS, HOT_EXPERTS - 1)
    cold_block = (jnp.maximum(slot_pos - HOT_EXPERTS * CAP_ROWS, 0) * n_cold) // cold_choices
    shifts = jax.random.randint(k_shift, (EXPERTS, 1), 0, n_cold)
    cold_rank = HOT_EXPERTS + (cold_block[None, :] + shifts) % n_cold
    rank_ids = jnp.where(slot_pos[None, :] < HOT_EXPERTS * CAP_ROWS, hot_rank[None, :], cold_rank)
    expert_perm = jax.random.permutation(k_perm, EXPERTS)
    choice_ids = expert_perm[rank_ids]
    pair_ids = jnp.stack([choice_ids[:, :TOKENS_DEV], choice_ids[:, TOKENS_DEV:]], axis=-1)
    token_perm = jax.random.permutation(k_order, jnp.tile(jnp.arange(TOKENS_DEV), (EXPERTS, 1)), axis=1, independent=True)
    pair_ids = jnp.take_along_axis(pair_ids, token_perm[:, :, None], axis=1)
    swap_bit = jax.random.randint(k_swap, (EXPERTS, TOKENS_DEV, 1), 0, 2)
    pair_ids = jnp.where(swap_bit == 1, pair_ids[:, :, ::-1], pair_ids)
    return pair_ids.reshape(ALL_TOKENS, 2).astype(jnp.int32)


def setup_inputs(seed: int = 0) -> dict:
    rng_key = jax.random.key(seed)
    k_tok, k_grad, k_route, k_gate, k_in, k_out = jax.random.split(rng_key, 6)
    tokens = jax.random.normal(k_tok, (ALL_TOKENS, D_MODEL), jnp.float32).astype(jnp.bfloat16)
    grad_out = jax.random.normal(k_grad, (ALL_TOKENS, D_MODEL), jnp.float32).astype(jnp.bfloat16)
    expert_ids = draw_routes(k_route)
    w_gate = (jax.random.normal(k_gate, (D_MODEL, EXPERTS), jnp.float32) * D_MODEL ** -0.5).astype(jnp.bfloat16)
    w_in = (jax.random.normal(k_in, (EXPERTS, D_MODEL, D_HIDDEN), jnp.float32) * D_MODEL ** -0.5).astype(jnp.bfloat16)
    w_out = (jax.random.normal(k_out, (EXPERTS, D_HIDDEN, D_MODEL), jnp.float32) * D_HIDDEN ** -0.5).astype(jnp.bfloat16)
    return {'tokens': tokens, 'grad_out': grad_out, 'expert_ids': expert_ids, 'w_gate': w_gate, 'w_in': w_in, 'w_out': w_out}


def reference(tokens, grad_out, expert_ids, w_gate, w_in, w_out):
    n_choice = 2 * ALL_TOKENS
    logits = jnp.dot(tokens, w_gate, preferred_element_type=jnp.float32)
    prob_all = jax.nn.softmax(logits, axis=-1)
    picked = jnp.take_along_axis(prob_all, expert_ids, axis=1)
    gate_val = picked / jnp.sum(picked, axis=1, keepdims=True)
    flat_ids = expert_ids.reshape(-1)
    sort_order = jnp.argsort(flat_ids, stable=True)
    counts = jnp.bincount(flat_ids, length=EXPERTS)
    starts = jnp.cumsum(counts) - counts
    pad_rows = jnp.zeros((CAP_ALL, D_MODEL), jnp.bfloat16)
    x_sorted = jnp.concatenate([tokens[sort_order // 2], pad_rows], axis=0)
    dy_flat = (gate_val[:, :, None] * grad_out[:, None, :].astype(jnp.float32)).astype(jnp.bfloat16).reshape(n_choice, D_MODEL)
    dy_sorted = jnp.concatenate([dy_flat[sort_order], pad_rows], axis=0)
    row_iota = jnp.arange(CAP_ALL)[:, None]

    def expert_step(scan_carry, per_expert):
        y_acc, dx_acc = scan_carry
        w_one, w_two, start_row, row_count = per_expert
        keep_row = row_iota < row_count
        x_rows = jnp.where(keep_row, lax.dynamic_slice_in_dim(x_sorted, start_row, CAP_ALL), 0)
        dy_rows = jnp.where(keep_row, lax.dynamic_slice_in_dim(dy_sorted, start_row, CAP_ALL), 0)
        a_pre = jnp.dot(x_rows, w_one, preferred_element_type=jnp.float32)
        hidden, gelu_vjp = jax.vjp(jax.nn.gelu, a_pre)
        hid_b = hidden.astype(jnp.bfloat16)
        y_rows = jnp.dot(hid_b, w_two, preferred_element_type=jnp.float32).astype(jnp.bfloat16)
        g_two = jnp.dot(hid_b.T, dy_rows, preferred_element_type=jnp.float32)
        d_hid = jnp.dot(dy_rows, w_two.T, preferred_element_type=jnp.float32)
        d_pre = gelu_vjp(d_hid)[0].astype(jnp.bfloat16)
        g_one = jnp.dot(x_rows.T, d_pre, preferred_element_type=jnp.float32)
        dx_rows = jnp.dot(d_pre, w_one.T, preferred_element_type=jnp.float32).astype(jnp.bfloat16)
        y_acc = lax.dynamic_update_slice_in_dim(y_acc, lax.dynamic_slice_in_dim(y_acc, start_row, CAP_ALL) + y_rows.astype(jnp.float32), start_row, axis=0)
        dx_acc = lax.dynamic_update_slice_in_dim(dx_acc, lax.dynamic_slice_in_dim(dx_acc, start_row, CAP_ALL) + dx_rows.astype(jnp.float32), start_row, axis=0)
        return (y_acc, dx_acc), (g_one, g_two)

    acc_init = jnp.zeros((n_choice + CAP_ALL, D_MODEL), jnp.float32)
    acc_done, grads = lax.scan(expert_step, (acc_init, acc_init), (w_in, w_out, starts, counts))
    g_in, g_out = grads
    y_sorted = acc_done[0][:n_choice]
    dx_sorted = acc_done[1][:n_choice]
    y_pair = jnp.zeros_like(y_sorted).at[sort_order].set(y_sorted).reshape(ALL_TOKENS, 2, D_MODEL)
    dx_pair = jnp.zeros_like(dx_sorted).at[sort_order].set(dx_sorted).reshape(ALL_TOKENS, 2, D_MODEL)
    y_out = jnp.sum(gate_val[:, :, None] * y_pair, axis=1).astype(jnp.bfloat16)
    d_gate = jnp.sum(grad_out.astype(jnp.float32)[:, None, :] * y_pair, axis=-1)
    d_sel = gate_val * (d_gate - jnp.sum(gate_val * d_gate, axis=1, keepdims=True))
    choice_hot = expert_ids[:, :, None] == jnp.arange(EXPERTS)[None, None, :]
    d_logits = jnp.sum(jnp.where(choice_hot, d_sel[:, :, None], 0.0), axis=1).astype(jnp.bfloat16)
    grad_x = (jnp.sum(dx_pair, axis=1) + jnp.dot(d_logits, w_gate.T, preferred_element_type=jnp.float32)).astype(jnp.bfloat16)
    grad_w_gate = jnp.dot(tokens.T, d_logits, preferred_element_type=jnp.float32)
    return y_out, grad_x, g_in, g_out, grad_w_gate
```

```python
import functools

import jax
import jax.numpy as jnp
from jax import lax
from jax.experimental import pallas as pl
from jax.experimental.pallas import tpu as pltpu
from jax.sharding import PartitionSpec as P

BASE = 104
EXTRA = 80
FULL = 256
F32 = jnp.float32
BF16 = jnp.bfloat16


def slot_of(ids, rank, base, extra):
    if not extra:
        return ids * base + rank
    block = base + extra
    over = rank - base
    second = (over >= extra).astype(jnp.int32)
    spill = ((ids & -2) + second) * block + base + over - second * extra
    return jnp.where(rank < base, ids * block + rank, spill)


def softmax_pair(l0, l1):
    top = jnp.maximum(l0, l1)
    e0 = jnp.exp(l0 - top)
    e1 = jnp.exp(l1 - top)
    tot = e0 + e1
    return e0 / tot, e1 / tot


def dispatch_kernel(base, extra, x_ref, do_ref, ids_ref, idst_ref, wg_ref, sx_ref, sdy_ref, slot_ref, gate_ref, slott_ref, gatet_ref):
    n_tok = x_ref.shape[0]
    n_exp = wg_ref.shape[1]
    step = pl.program_id(0)
    rows = base + extra

    @pl.when(step == 0)
    def _():
        r_i = lax.broadcasted_iota(jnp.int32, (n_tok, n_tok), 0)
        c_i = lax.broadcasted_iota(jnp.int32, (n_tok, n_tok), 1)
        e_col = lax.broadcasted_iota(jnp.int32, (n_tok, n_exp), 1)
        id0, id1 = ids_ref[:, 0:1], ids_ref[:, 1:2]
        h0, h1 = id0 == e_col, id1 == e_col
        lower = jnp.where(c_i < r_i, 1.0, 0.0).astype(BF16)
        named = jnp.where(h0 | h1, 1.0, 0.0).astype(BF16)
        before = jnp.dot(lower, named, preferred_element_type=F32)
        logits = jnp.dot(x_ref[...], wg_ref[...], preferred_element_type=F32)
        pick = lambda hot, val: jnp.sum(jnp.where(hot, val, 0.0), axis=1, keepdims=True)
        slot_ref[:, 0:1] = slot_of(id0, pick(h0, before).astype(jnp.int32), base, extra)
        slot_ref[:, 1:2] = slot_of(id1, pick(h1, before).astype(jnp.int32), base, extra)
        g0, g1 = softmax_pair(pick(h0, logits), pick(h1, logits))
        gate_ref[:, 0:1] = g0
        gate_ref[:, 1:2] = g1
        e_row = lax.broadcasted_iota(jnp.int32, (n_exp, n_tok), 0)
        it0, it1 = idst_ref[0:1, :], idst_ref[1:2, :]
        t0, t1 = it0 == e_row, it1 == e_row
        upper = jnp.where(r_i < c_i, 1.0, 0.0).astype(BF16)
        named_t = jnp.where(t0 | t1, 1.0, 0.0).astype(BF16)
        before_t = jnp.dot(named_t, upper, preferred_element_type=F32)
        logits_t = lax.dot_general(wg_ref[...], x_ref[...], (((0,), (1,)), ((), ())), preferred_element_type=F32)
        pick_t = lambda hot, val: jnp.sum(jnp.where(hot, val, 0.0), axis=0, keepdims=True)
        slott_ref[0:1, :] = slot_of(it0, pick_t(t0, before_t).astype(jnp.int32), base, extra)
        slott_ref[1:2, :] = slot_of(it1, pick_t(t1, before_t).astype(jnp.int32), base, extra)
        g0t, g1t = softmax_pair(pick_t(t0, logits_t), pick_t(t1, logits_t))
        gatet_ref[0:1, :] = g0t
        gatet_ref[1:2, :] = g1t

    row = step * rows + lax.broadcasted_iota(jnp.int32, (rows, n_tok), 0)
    d0 = slott_ref[0:1, :] == row
    d1 = slott_ref[1:2, :] == row
    sel = jnp.where(d0 | d1, 1.0, 0.0).astype(BF16)
    g_row = jnp.sum(jnp.where(d0, gatet_ref[0:1, :], 0.0) + jnp.where(d1, gatet_ref[1:2, :], 0.0), axis=1, keepdims=True)
    sx_ref[0] = jnp.dot(sel, x_ref[...], preferred_element_type=F32).astype(BF16)
    sdy_ref[0] = (g_row * jnp.dot(sel, do_ref[...], preferred_element_type=F32)).astype(BF16)


def dispatch(tokens, grad_out, ids, w_gate, base, extra):
    n_tok, d_model = tokens.shape
    n_exp = w_gate.shape[1]
    rows = base + extra
    whole = lambda shape: pl.BlockSpec(shape, lambda i: (0,) * len(shape))
    block = pl.BlockSpec((1, rows, d_model), lambda i: (i, 0, 0))
    send = jax.ShapeDtypeStruct((n_exp, rows, d_model), BF16)
    return pl.pallas_call(
        functools.partial(dispatch_kernel, base, extra),
        grid=(n_exp,),
        in_specs=[whole((n_tok, d_model)), whole((n_tok, d_model)), whole((n_tok, 2)), whole((2, n_tok)), whole((d_model, n_exp))],
        out_specs=[block, block, whole((n_tok, 2)), whole((n_tok, 2))],
        out_shape=[send, send, jax.ShapeDtypeStruct((n_tok, 2), jnp.int32), jax.ShapeDtypeStruct((n_tok, 2), F32)],
        scratch_shapes=[pltpu.VMEM((2, n_tok), jnp.int32), pltpu.VMEM((2, n_tok), F32)],
        compiler_params=pltpu.CompilerParams(vmem_limit_bytes=56 * 2 ** 20),
        cost_estimate=pl.CostEstimate(flops=4 * n_exp * rows * n_tok * d_model, bytes_accessed=4 * n_exp * rows * d_model, transcendentals=0),
        name='dispatch',
    )(tokens, grad_out, ids, ids.T, w_gate)


def gather_y_kernel(y_ref, do_ref, x_ref, ids_ref, slot_ref, gate_ref, out_ref, dl_ref, gw_ref):
    n_tile = do_ref.shape[0]
    n_exp = dl_ref.shape[1]
    col = lax.broadcasted_iota(jnp.int32, (n_tile, y_ref.shape[0]), 1)
    s0 = jnp.where(slot_ref[:, 0:1] == col, 1.0, 0.0).astype(BF16)
    s1 = jnp.where(slot_ref[:, 1:2] == col, 1.0, 0.0).astype(BF16)
    y0 = jnp.dot(s0, y_ref[...], preferred_element_type=F32)
    y1 = jnp.dot(s1, y_ref[...], preferred_element_type=F32)
    g0, g1 = gate_ref[:, 0:1], gate_ref[:, 1:2]
    out_ref[...] = (g0 * y0 + g1 * y1).astype(BF16)
    do = do_ref[...].astype(F32)
    dg0 = jnp.sum(do * y0, axis=1, keepdims=True)
    dg1 = jnp.sum(do * y1, axis=1, keepdims=True)
    mean = g0 * dg0 + g1 * dg1
    e_col = lax.broadcasted_iota(jnp.int32, (n_tile, n_exp), 1)
    dl = jnp.where(ids_ref[:, 0:1] == e_col, g0 * (dg0 - mean), 0.0) + jnp.where(ids_ref[:, 1:2] == e_col, g1 * (dg1 - mean), 0.0)
    dl = dl.astype(BF16)
    dl_ref[...] = dl

    @pl.when(pl.program_id(0) == 0)
    def _():
        gw_ref[...] = jnp.zeros_like(gw_ref)

    gw_ref[...] += lax.dot_general(x_ref[...], dl, (((0,), (0,)), ((), ())), preferred_element_type=F32)


def gather_y(y_back, grad_out, tokens, ids, slots, gates, n_exp):
    n_tok, d_model = tokens.shape
    n_slot = y_back.shape[0]
    tile = 256
    per = lambda width: pl.BlockSpec((tile, width), lambda i: (i, 0))
    return pl.pallas_call(
        gather_y_kernel,
        grid=(n_tok // tile,),
        in_specs=[pl.BlockSpec((n_slot, d_model), lambda i: (0, 0)), per(d_model), per(d_model), per(2), per(2), per(2)],
        out_specs=[per(d_model), per(n_exp), pl.BlockSpec((d_model, n_exp), lambda i: (0, 0))],
        out_shape=[jax.ShapeDtypeStruct((n_tok, d_model), BF16), jax.ShapeDtypeStruct((n_tok, n_exp), BF16), jax.ShapeDtypeStruct((d_model, n_exp), F32)],
        compiler_params=pltpu.CompilerParams(vmem_limit_bytes=56 * 2 ** 20),
        cost_estimate=pl.CostEstimate(flops=4 * n_slot * n_tok * d_model, bytes_accessed=2 * n_slot * d_model, transcendentals=0),
        name='gather_y',
    )(y_back, grad_out, tokens, ids, slots, gates)


def gather_dx_kernel(dx_ref, dl_ref, wg_ref, slot_ref, out_ref):
    col = lax.broadcasted_iota(jnp.int32, (out_ref.shape[0], dx_ref.shape[0]), 1)
    sel = jnp.where((slot_ref[:, 0:1] == col) | (slot_ref[:, 1:2] == col), 1.0, 0.0).astype(BF16)
    tot = jnp.dot(sel, dx_ref[...], preferred_element_type=F32)
    tot += lax.dot_general(dl_ref[...], wg_ref[...], (((1,), (1,)), ((), ())), preferred_element_type=F32)
    out_ref[...] = tot.astype(BF16)


def gather_dx(dx_back, d_logits, w_gate, slots):
    n_tok, n_exp = d_logits.shape
    n_slot, d_model = dx_back.shape
    tile = 256
    per = lambda width: pl.BlockSpec((tile, width), lambda i: (i, 0))
    return pl.pallas_call(
        gather_dx_kernel,
        grid=(n_tok // tile,),
        in_specs=[pl.BlockSpec((n_slot, d_model), lambda i: (0, 0)), per(n_exp), pl.BlockSpec((d_model, n_exp), lambda i: (0, 0)), per(2)],
        out_specs=per(d_model),
        out_shape=jax.ShapeDtypeStruct((n_tok, d_model), BF16),
        compiler_params=pltpu.CompilerParams(vmem_limit_bytes=56 * 2 ** 20),
        cost_estimate=pl.CostEstimate(flops=2 * n_slot * n_tok * d_model, bytes_accessed=2 * n_slot * d_model, transcendentals=0),
        name='gather_dx',
    )(dx_back, d_logits, w_gate, slots)


def swap(value, n_dev):
    return lax.ppermute(value, 'ep', [(d, d ^ 1) for d in range(n_dev)])


def exchange(value):
    return lax.all_to_all(value, 'ep', 0, 0, tiled=True)


def expert_fwd(rows, w_one, w_two):
    a_pre = jnp.dot(rows, w_one, preferred_element_type=F32)
    hidden, gelu_vjp = jax.vjp(jax.nn.gelu, a_pre)
    hid_b = hidden.astype(BF16)
    y_rows = jnp.dot(hid_b, w_two, preferred_element_type=F32).astype(BF16)
    return hid_b, gelu_vjp, y_rows


def expert_bwd(dy_rows, gelu_vjp, w_one, w_two):
    d_hid = jnp.einsum('rm,hm->rh', dy_rows, w_two, preferred_element_type=F32)
    d_pre = gelu_vjp(d_hid)[0].astype(BF16)
    return d_pre, jnp.einsum('rh,mh->rm', d_pre, w_one, preferred_element_type=F32).astype(BF16)


def weight_grads(rows, hid_b, dy_rows, d_pre):
    g_two = jnp.einsum('rh,rm->hm', hid_b, dy_rows, preferred_element_type=F32)
    g_one = jnp.einsum('rm,rh->mh', rows, d_pre, preferred_element_type=F32)
    return g_one, g_two


def run_path(base, extra, tokens, grad_out, ids, w_gate, w_one, w_two, mine):
    n_exp = w_gate.shape[1]
    d_model = tokens.shape[1]
    rows = base + extra
    send_x, send_dy, slots, gates = dispatch(tokens, grad_out, ids, w_gate, base, extra)
    recv_x = exchange(send_x)
    recv_dy = exchange(send_dy)
    first = lambda v: v[:, :base].reshape(n_exp * base, d_model)
    x_b, dy_b = first(recv_x), first(recv_dy)
    hid_b, vjp_b, y_b = expert_fwd(x_b, w_one, w_two)
    if extra:
        last = lambda v: v[:, base:].reshape(n_exp * extra, d_model)
        x_e, dy_e = last(recv_x), last(recv_dy)
        hot_one = jnp.where(mine, w_one, swap(w_one, n_exp))
        hot_two = jnp.where(mine, w_two, swap(w_two, n_exp))
        hid_e, vjp_e, y_e = expert_fwd(x_e, hot_one, hot_two)
        y_rows = jnp.concatenate([y_b.reshape(n_exp, base, d_model), y_e.reshape(n_exp, extra, d_model)], axis=1)
    else:
        y_rows = y_b.reshape(n_exp, base, d_model)
    y_back = exchange(y_rows).reshape(n_exp * rows, d_model)
    dp_b, dx_b = expert_bwd(dy_b, vjp_b, w_one, w_two)
    if extra:
        dp_e, dx_e = expert_bwd(dy_e, vjp_e, hot_one, hot_two)
        dx_rows = jnp.concatenate([dx_b.reshape(n_exp, base, d_model), dx_e.reshape(n_exp, extra, d_model)], axis=1)
    else:
        dx_rows = dx_b.reshape(n_exp, base, d_model)
    dx_back = exchange(dx_rows).reshape(n_exp * rows, d_model)
    g_one, g_two = weight_grads(x_b, hid_b, dy_b, dp_b)
    if extra:
        e_one, e_two = weight_grads(x_e, hid_e, dy_e, dp_e)
        keep = jnp.where(mine, 1.0, 0.0)
        g_one = g_one + keep * (e_one + swap(e_one, n_exp))
        g_two = g_two + keep * (e_two + swap(e_two, n_exp))
    y_out, d_logits, gw_part = gather_y(y_back, grad_out, tokens, ids, slots, gates, n_exp)
    grad_w_gate = lax.psum(gw_part, 'ep')
    grad_x = gather_dx(dx_back, d_logits, w_gate, slots)
    return y_out, grad_x, g_one, g_two, grad_w_gate


def local_block(tokens, grad_out, expert_ids, w_gate, w_in, w_out):
    n_exp = w_gate.shape[1]
    me = lax.axis_index('ep')
    counts = jnp.sum((expert_ids.reshape(-1)[:, None] == jnp.arange(n_exp)[None, :]).astype(jnp.int32), axis=0)
    most = lax.pmax(counts, 'ep')
    over = most > BASE
    mine = over[me]
    both = jnp.any(over.reshape(n_exp // 2, 2).all(axis=1))
    args = (tokens, grad_out, expert_ids, w_gate, w_in[0], w_out[0], mine)
    y_out, grad_x, g_one, g_two, g_gate = lax.cond(both, functools.partial(run_path, FULL, 0), functools.partial(run_path, BASE, EXTRA), *args)
    return y_out, grad_x, g_one[None], g_two[None], g_gate


def solution(mesh):
    return jax.shard_map(local_block, mesh=mesh, in_specs=(P('ep'), P('ep'), P('ep'), P(), P('ep'), P('ep')), out_specs=(P('ep'), P('ep'), P('ep'), P('ep'), P()), check_vma=False)
```

```python
import functools

import jax
import jax.numpy as jnp
from jax import lax
from jax.experimental import pallas as pl
from jax.experimental.pallas import tpu as pltpu
from jax.sharding import PartitionSpec as P

BASE = 112
EXTRA = 80
FULL = 256
F32 = jnp.float32
BF16 = jnp.bfloat16


def slot_of(ids, rank, base, extra):
    if not extra:
        return ids * base + rank
    block = base + extra
    over = rank - base
    second = (over >= extra).astype(jnp.int32)
    spill = ((ids & -2) + second) * block + base + over - second * extra
    return jnp.where(rank < base, ids * block + rank, spill)


def softmax_pair(l0, l1):
    top = jnp.maximum(l0, l1)
    e0 = jnp.exp(l0 - top)
    e1 = jnp.exp(l1 - top)
    tot = e0 + e1
    return e0 / tot, e1 / tot


def peer_copy(src, dst, send_sem, recv_sem, peer):
    return pltpu.make_async_remote_copy(src_ref=src, dst_ref=dst, send_sem=send_sem, recv_sem=recv_sem, device_id=(peer,), device_id_type=pl.DeviceIdType.MESH)


def share_counts(cnt_ref, all_ref, send_sem, recv_sem, n_dev):
    me = lax.axis_index('ep')
    return [peer_copy(cnt_ref, all_ref.at[me], send_sem.at[i], recv_sem.at[i], lax.rem(me + i, n_dev)) for i in range(1, n_dev)]


def dispatch_kernel(base, extra, share, x_ref, do_ref, ids_ref, idst_ref, wg_ref, sx_ref, sdy_ref, slot_ref, gate_ref, *rest):
    n_tok = x_ref.shape[0]
    n_exp = wg_ref.shape[1]
    step = pl.program_id(0)
    rows = base + extra
    if share:
        most_ref, slott_ref, gatet_ref, cnt_ref, all_ref, send_sem, recv_sem = rest
    else:
        slott_ref, gatet_ref = rest

    @pl.when(step == 0)
    def _():
        r_i = lax.broadcasted_iota(jnp.int32, (n_tok, n_tok), 0)
        c_i = lax.broadcasted_iota(jnp.int32, (n_tok, n_tok), 1)
        e_col = lax.broadcasted_iota(jnp.int32, (n_tok, n_exp), 1)
        id0, id1 = ids_ref[:, 0:1], ids_ref[:, 1:2]
        h0, h1 = id0 == e_col, id1 == e_col
        lower = jnp.where(c_i < r_i, 1.0, 0.0).astype(BF16)
        named = jnp.where(h0 | h1, 1.0, 0.0).astype(BF16)
        if share:
            cnt_ref[...] = jnp.zeros_like(cnt_ref)
            cnt_ref[0:1, 0:n_exp] = jnp.sum(named.astype(F32), axis=0, keepdims=True)
            for copy in share_counts(cnt_ref, all_ref, send_sem, recv_sem, n_exp):
                copy.start()
        before = jnp.dot(lower, named, preferred_element_type=F32)
        logits = jnp.dot(x_ref[...], wg_ref[...], preferred_element_type=F32)
        pick = lambda hot, val: jnp.sum(jnp.where(hot, val, 0.0), axis=1, keepdims=True)
        slot_ref[:, 0:1] = slot_of(id0, pick(h0, before).astype(jnp.int32), base, extra)
        slot_ref[:, 1:2] = slot_of(id1, pick(h1, before).astype(jnp.int32), base, extra)
        g0, g1 = softmax_pair(pick(h0, logits), pick(h1, logits))
        gate_ref[:, 0:1] = g0
        gate_ref[:, 1:2] = g1
        e_row = lax.broadcasted_iota(jnp.int32, (n_exp, n_tok), 0)
        it0, it1 = idst_ref[0:1, :], idst_ref[1:2, :]
        t0, t1 = it0 == e_row, it1 == e_row
        upper = jnp.where(r_i < c_i, 1.0, 0.0).astype(BF16)
        named_t = jnp.where(t0 | t1, 1.0, 0.0).astype(BF16)
        before_t = jnp.dot(named_t, upper, preferred_element_type=F32)
        logits_t = lax.dot_general(wg_ref[...], x_ref[...], (((0,), (1,)), ((), ())), preferred_element_type=F32)
        pick_t = lambda hot, val: jnp.sum(jnp.where(hot, val, 0.0), axis=0, keepdims=True)
        slott_ref[0:1, :] = slot_of(it0, pick_t(t0, before_t).astype(jnp.int32), base, extra)
        slott_ref[1:2, :] = slot_of(it1, pick_t(t1, before_t).astype(jnp.int32), base, extra)
        g0t, g1t = softmax_pair(pick_t(t0, logits_t), pick_t(t1, logits_t))
        gatet_ref[0:1, :] = g0t
        gatet_ref[1:2, :] = g1t

    row = step * rows + lax.broadcasted_iota(jnp.int32, (rows, n_tok), 0)
    d0 = slott_ref[0:1, :] == row
    d1 = slott_ref[1:2, :] == row
    sel = jnp.where(d0 | d1, 1.0, 0.0).astype(BF16)
    g_row = jnp.sum(jnp.where(d0, gatet_ref[0:1, :], 0.0) + jnp.where(d1, gatet_ref[1:2, :], 0.0), axis=1, keepdims=True)
    sx_ref[0] = jnp.dot(sel, x_ref[...], preferred_element_type=F32).astype(BF16)
    sdy_ref[0] = (g_row * jnp.dot(sel, do_ref[...], preferred_element_type=F32)).astype(BF16)

    if share:
        @pl.when(step == n_exp - 1)
        def _():
            for copy in share_counts(cnt_ref, all_ref, send_sem, recv_sem, n_exp):
                copy.wait()
            all_ref[lax.axis_index('ep')] = cnt_ref[...]
            most_ref[...] = jnp.max(all_ref[...], axis=0)


def dispatch(tokens, grad_out, ids, w_gate, base, extra, share):
    n_tok, d_model = tokens.shape
    n_exp = w_gate.shape[1]
    rows = base + extra
    whole = lambda shape: pl.BlockSpec(shape, lambda i: (0,) * len(shape))
    block = pl.BlockSpec((1, rows, d_model), lambda i: (i, 0, 0))
    send = jax.ShapeDtypeStruct((n_exp, rows, d_model), BF16)
    out_specs = [block, block, whole((n_tok, 2)), whole((n_tok, 2))]
    out_shape = [send, send, jax.ShapeDtypeStruct((n_tok, 2), jnp.int32), jax.ShapeDtypeStruct((n_tok, 2), F32)]
    scratch = [pltpu.VMEM((2, n_tok), jnp.int32), pltpu.VMEM((2, n_tok), F32)]
    if share:
        out_specs.append(whole((8, 128)))
        out_shape.append(jax.ShapeDtypeStruct((8, 128), F32))
        scratch += [pltpu.VMEM((8, 128), F32), pltpu.VMEM((n_exp, 8, 128), F32), pltpu.SemaphoreType.DMA((n_exp,)), pltpu.SemaphoreType.DMA((n_exp,))]
    return pl.pallas_call(
        functools.partial(dispatch_kernel, base, extra, share),
        grid=(n_exp,),
        in_specs=[whole((n_tok, d_model)), whole((n_tok, d_model)), whole((n_tok, 2)), whole((2, n_tok)), whole((d_model, n_exp))],
        out_specs=out_specs,
        out_shape=out_shape,
        scratch_shapes=scratch,
        compiler_params=pltpu.CompilerParams(vmem_limit_bytes=56 * 2 ** 20, has_side_effects=share),
        cost_estimate=pl.CostEstimate(flops=4 * n_exp * rows * n_tok * d_model, bytes_accessed=4 * n_exp * rows * d_model, transcendentals=0),
        name='dispatch',
    )(tokens, grad_out, ids, ids.T, w_gate)


def gather_y_kernel(y_ref, do_ref, x_ref, ids_ref, slot_ref, gate_ref, out_ref, dl_ref, gw_ref):
    n_tile = do_ref.shape[0]
    n_exp = dl_ref.shape[1]
    col = lax.broadcasted_iota(jnp.int32, (n_tile, y_ref.shape[0]), 1)
    s0 = jnp.where(slot_ref[:, 0:1] == col, 1.0, 0.0).astype(BF16)
    s1 = jnp.where(slot_ref[:, 1:2] == col, 1.0, 0.0).astype(BF16)
    y0 = jnp.dot(s0, y_ref[...], preferred_element_type=F32)
    y1 = jnp.dot(s1, y_ref[...], preferred_element_type=F32)
    g0, g1 = gate_ref[:, 0:1], gate_ref[:, 1:2]
    out_ref[...] = (g0 * y0 + g1 * y1).astype(BF16)
    do = do_ref[...].astype(F32)
    dg0 = jnp.sum(do * y0, axis=1, keepdims=True)
    dg1 = jnp.sum(do * y1, axis=1, keepdims=True)
    mean = g0 * dg0 + g1 * dg1
    e_col = lax.broadcasted_iota(jnp.int32, (n_tile, n_exp), 1)
    dl = jnp.where(ids_ref[:, 0:1] == e_col, g0 * (dg0 - mean), 0.0) + jnp.where(ids_ref[:, 1:2] == e_col, g1 * (dg1 - mean), 0.0)
    dl = dl.astype(BF16)
    dl_ref[...] = dl

    @pl.when(pl.program_id(0) == 0)
    def _():
        gw_ref[...] = jnp.zeros_like(gw_ref)

    gw_ref[...] += lax.dot_general(x_ref[...], dl, (((0,), (0,)), ((), ())), preferred_element_type=F32)


def gather_y(y_back, grad_out, tokens, ids, slots, gates, n_exp):
    n_tok, d_model = tokens.shape
    n_slot = y_back.shape[0]
    tile = 256
    per = lambda width: pl.BlockSpec((tile, width), lambda i: (i, 0))
    return pl.pallas_call(
        gather_y_kernel,
        grid=(n_tok // tile,),
        in_specs=[pl.BlockSpec((n_slot, d_model), lambda i: (0, 0)), per(d_model), per(d_model), per(2), per(2), per(2)],
        out_specs=[per(d_model), per(n_exp), pl.BlockSpec((d_model, n_exp), lambda i: (0, 0))],
        out_shape=[jax.ShapeDtypeStruct((n_tok, d_model), BF16), jax.ShapeDtypeStruct((n_tok, n_exp), BF16), jax.ShapeDtypeStruct((d_model, n_exp), F32)],
        compiler_params=pltpu.CompilerParams(vmem_limit_bytes=56 * 2 ** 20),
        cost_estimate=pl.CostEstimate(flops=4 * n_slot * n_tok * d_model, bytes_accessed=2 * n_slot * d_model, transcendentals=0),
        name='gather_y',
    )(y_back, grad_out, tokens, ids, slots, gates)


def gather_dx_kernel(dx_ref, dl_ref, wg_ref, slot_ref, out_ref):
    col = lax.broadcasted_iota(jnp.int32, (out_ref.shape[0], dx_ref.shape[0]), 1)
    sel = jnp.where((slot_ref[:, 0:1] == col) | (slot_ref[:, 1:2] == col), 1.0, 0.0).astype(BF16)
    tot = jnp.dot(sel, dx_ref[...], preferred_element_type=F32)
    tot += lax.dot_general(dl_ref[...], wg_ref[...], (((1,), (1,)), ((), ())), preferred_element_type=F32)
    out_ref[...] = tot.astype(BF16)


def gather_dx(dx_back, d_logits, w_gate, slots):
    n_tok, n_exp = d_logits.shape
    n_slot, d_model = dx_back.shape
    tile = 256
    per = lambda width: pl.BlockSpec((tile, width), lambda i: (i, 0))
    return pl.pallas_call(
        gather_dx_kernel,
        grid=(n_tok // tile,),
        in_specs=[pl.BlockSpec((n_slot, d_model), lambda i: (0, 0)), per(n_exp), pl.BlockSpec((d_model, n_exp), lambda i: (0, 0)), per(2)],
        out_specs=per(d_model),
        out_shape=jax.ShapeDtypeStruct((n_tok, d_model), BF16),
        compiler_params=pltpu.CompilerParams(vmem_limit_bytes=56 * 2 ** 20),
        cost_estimate=pl.CostEstimate(flops=2 * n_slot * n_tok * d_model, bytes_accessed=2 * n_slot * d_model, transcendentals=0),
        name='gather_dx',
    )(dx_back, d_logits, w_gate, slots)


def gate_sum_kernel(part_ref, out_ref, all_ref, send_sem, recv_sem):
    n_dev = part_ref.shape[0]
    me = lax.axis_index('ep')
    peers = [(i, lax.rem(me + i, n_dev)) for i in range(1, n_dev)]
    first = [peer_copy(part_ref.at[d], all_ref.at[me], send_sem.at[0, i], recv_sem.at[0, i], d) for i, d in peers]
    for copy in first:
        copy.start()
    all_ref[me] = part_ref[me]
    for copy in first:
        copy.wait()
    out_ref[me] = jnp.sum(all_ref[...], axis=0)
    second = [peer_copy(out_ref.at[me], out_ref.at[me], send_sem.at[1, i], recv_sem.at[1, i], d) for i, d in peers]
    for copy in second:
        copy.start()
    for copy in second:
        copy.wait()


def gate_sum(part):
    d_model, n_exp = part.shape
    tiles = jnp.pad(part.reshape(n_exp, -1, 128), ((0, 0), (0, 2), (0, 0)))
    vmem = pl.BlockSpec(memory_space=pltpu.VMEM)
    total = pl.pallas_call(
        gate_sum_kernel,
        in_specs=[vmem],
        out_specs=vmem,
        out_shape=jax.ShapeDtypeStruct(tiles.shape, F32),
        scratch_shapes=[pltpu.VMEM(tiles.shape, F32), pltpu.SemaphoreType.DMA((2, n_exp)), pltpu.SemaphoreType.DMA((2, n_exp))],
        compiler_params=pltpu.CompilerParams(has_side_effects=True),
        name='gate_sum',
    )(tiles)
    return total[:, :6].reshape(d_model, n_exp)


def swap(value, n_dev):
    return lax.ppermute(value, 'ep', [(d, d ^ 1) for d in range(n_dev)])


def exchange(value):
    return lax.all_to_all(value, 'ep', 0, 0, tiled=True)


def expert_fwd(rows, w_one, w_two):
    a_pre = jnp.dot(rows, w_one, preferred_element_type=F32)
    hidden, gelu_vjp = jax.vjp(jax.nn.gelu, a_pre)
    hid_b = hidden.astype(BF16)
    y_rows = jnp.dot(hid_b, w_two, preferred_element_type=F32).astype(BF16)
    return hid_b, gelu_vjp, y_rows


def expert_bwd(dy_rows, gelu_vjp, w_one, w_two):
    d_hid = jnp.einsum('rm,hm->rh', dy_rows, w_two, preferred_element_type=F32)
    d_pre = gelu_vjp(d_hid)[0].astype(BF16)
    return d_pre, jnp.einsum('rh,mh->rm', d_pre, w_one, preferred_element_type=F32).astype(BF16)


def weight_grads(rows, hid_b, dy_rows, d_pre):
    g_two = jnp.einsum('rh,rm->hm', hid_b, dy_rows, preferred_element_type=F32)
    g_one = jnp.einsum('rm,rh->mh', rows, d_pre, preferred_element_type=F32)
    return g_one, g_two


def padded_path(tokens, grad_out, ids, w_gate, w_one, w_two, mine, *sent):
    sent = dispatch(tokens, grad_out, ids, w_gate, FULL, 0, False)
    return run_path(FULL, 0, tokens, grad_out, ids, w_gate, w_one, w_two, mine, *sent)


def run_path(base, extra, tokens, grad_out, ids, w_gate, w_one, w_two, mine, send_x, send_dy, slots, gates):
    n_exp = w_gate.shape[1]
    d_model = tokens.shape[1]
    rows = base + extra
    recv_x = exchange(send_x)
    recv_dy = exchange(send_dy)
    first = lambda v: v[:, :base].reshape(n_exp * base, d_model)
    x_b, dy_b = first(recv_x), first(recv_dy)
    hid_b, vjp_b, y_b = expert_fwd(x_b, w_one, w_two)
    if extra:
        last = lambda v: v[:, base:].reshape(n_exp * extra, d_model)
        x_e, dy_e = last(recv_x), last(recv_dy)
        hot_one = jnp.where(mine, w_one, swap(w_one, n_exp))
        hot_two = jnp.where(mine, w_two, swap(w_two, n_exp))
        hid_e, vjp_e, y_e = expert_fwd(x_e, hot_one, hot_two)
        y_rows = jnp.concatenate([y_b.reshape(n_exp, base, d_model), y_e.reshape(n_exp, extra, d_model)], axis=1)
    else:
        y_rows = y_b.reshape(n_exp, base, d_model)
    y_back = exchange(y_rows).reshape(n_exp * rows, d_model)
    dp_b, dx_b = expert_bwd(dy_b, vjp_b, w_one, w_two)
    if extra:
        dp_e, dx_e = expert_bwd(dy_e, vjp_e, hot_one, hot_two)
        dx_rows = jnp.concatenate([dx_b.reshape(n_exp, base, d_model), dx_e.reshape(n_exp, extra, d_model)], axis=1)
    else:
        dx_rows = dx_b.reshape(n_exp, base, d_model)
    dx_back = exchange(dx_rows).reshape(n_exp * rows, d_model)
    g_one, g_two = weight_grads(x_b, hid_b, dy_b, dp_b)
    if extra:
        e_one, e_two = weight_grads(x_e, hid_e, dy_e, dp_e)
        keep = jnp.where(mine, 1.0, 0.0)
        g_one = g_one + keep * (e_one + swap(e_one, n_exp))
        g_two = g_two + keep * (e_two + swap(e_two, n_exp))
    y_out, d_logits, gw_part = gather_y(y_back, grad_out, tokens, ids, slots, gates, n_exp)
    grad_w_gate = gate_sum(gw_part)
    grad_x = gather_dx(dx_back, d_logits, w_gate, slots)
    return y_out, grad_x, g_one, g_two, grad_w_gate


def local_block(tokens, grad_out, expert_ids, w_gate, w_in, w_out):
    n_exp = w_gate.shape[1]
    *sent, most = dispatch(tokens, grad_out, expert_ids, w_gate, BASE, EXTRA, True)
    over = most[0, :n_exp] > BASE
    mine = over[lax.axis_index('ep')]
    both = jnp.any(over.reshape(n_exp // 2, 2).all(axis=1))
    args = (tokens, grad_out, expert_ids, w_gate, w_in[0], w_out[0], mine, *sent)
    y_out, grad_x, g_one, g_two, g_gate = lax.cond(both, padded_path, functools.partial(run_path, BASE, EXTRA), *args)
    return y_out, grad_x, g_one[None], g_two[None], g_gate


def solution(mesh):
    return jax.shard_map(local_block, mesh=mesh, in_specs=(P('ep'), P('ep'), P('ep'), P(), P('ep'), P('ep')), out_specs=(P('ep'), P('ep'), P('ep'), P('ep'), P()), check_vma=False)
```

```python
import functools

import jax
import jax.numpy as jnp
from jax import lax
from jax.experimental import pallas as pl
from jax.experimental.pallas import tpu as pltpu
from jax.sharding import PartitionSpec as P

BASE = 112
EXTRA = 80
FULL = 256
F32 = jnp.float32
BF16 = jnp.bfloat16


def slot_of(ids, rank, base, extra):
    if not extra:
        return ids * base + rank
    block = base + extra
    over = rank - base
    second = (over >= extra).astype(jnp.int32)
    spill = ((ids & -2) + second) * block + base + over - second * extra
    return jnp.where(rank < base, ids * block + rank, spill)


def softmax_pair(l0, l1):
    top = jnp.maximum(l0, l1)
    e0 = jnp.exp(l0 - top)
    e1 = jnp.exp(l1 - top)
    tot = e0 + e1
    return e0 / tot, e1 / tot


def peer_copy(src, dst, send_sem, recv_sem, peer):
    return pltpu.make_async_remote_copy(src_ref=src, dst_ref=dst, send_sem=send_sem, recv_sem=recv_sem, device_id=(peer,), device_id_type=pl.DeviceIdType.MESH)


def share_counts(cnt_ref, all_ref, send_sem, recv_sem, n_dev):
    me = lax.axis_index('ep')
    return [peer_copy(cnt_ref, all_ref.at[me], send_sem.at[i], recv_sem.at[i], lax.rem(me + i, n_dev)) for i in range(1, n_dev)]


def dispatch_kernel(base, extra, share, x_ref, do_ref, ids_ref, idst_ref, wg_ref, sx_ref, sdy_ref, slot_ref, gate_ref, *rest):
    n_tok = x_ref.shape[0]
    n_exp = wg_ref.shape[1]
    step = pl.program_id(0)
    rows = base + extra
    if share:
        most_ref, slott_ref, gatet_ref, cnt_ref, all_ref, send_sem, recv_sem = rest
    else:
        slott_ref, gatet_ref = rest

    @pl.when(step == 0)
    def _():
        r_i = lax.broadcasted_iota(jnp.int32, (n_tok, n_tok), 0)
        c_i = lax.broadcasted_iota(jnp.int32, (n_tok, n_tok), 1)
        e_col = lax.broadcasted_iota(jnp.int32, (n_tok, n_exp), 1)
        id0, id1 = ids_ref[:, 0:1], ids_ref[:, 1:2]
        h0, h1 = id0 == e_col, id1 == e_col
        lower = jnp.where(c_i < r_i, 1.0, 0.0).astype(BF16)
        named = jnp.where(h0 | h1, 1.0, 0.0).astype(BF16)
        if share:
            cnt_ref[...] = jnp.zeros_like(cnt_ref)
            cnt_ref[0:1, 0:n_exp] = jnp.sum(named.astype(F32), axis=0, keepdims=True)
            for copy in share_counts(cnt_ref, all_ref, send_sem, recv_sem, n_exp):
                copy.start()
        before = jnp.dot(lower, named, preferred_element_type=F32)
        logits = jnp.dot(x_ref[...], wg_ref[...], preferred_element_type=F32)
        pick = lambda hot, val: jnp.sum(jnp.where(hot, val, 0.0), axis=1, keepdims=True)
        slot_ref[:, 0:1] = slot_of(id0, pick(h0, before).astype(jnp.int32), base, extra)
        slot_ref[:, 1:2] = slot_of(id1, pick(h1, before).astype(jnp.int32), base, extra)
        g0, g1 = softmax_pair(pick(h0, logits), pick(h1, logits))
        gate_ref[:, 0:1] = g0
        gate_ref[:, 1:2] = g1
        e_row = lax.broadcasted_iota(jnp.int32, (n_exp, n_tok), 0)
        it0, it1 = idst_ref[0:1, :], idst_ref[1:2, :]
        t0, t1 = it0 == e_row, it1 == e_row
        upper = jnp.where(r_i < c_i, 1.0, 0.0).astype(BF16)
        named_t = jnp.where(t0 | t1, 1.0, 0.0).astype(BF16)
        before_t = jnp.dot(named_t, upper, preferred_element_type=F32)
        logits_t = lax.dot_general(wg_ref[...], x_ref[...], (((0,), (1,)), ((), ())), preferred_element_type=F32)
        pick_t = lambda hot, val: jnp.sum(jnp.where(hot, val, 0.0), axis=0, keepdims=True)
        slott_ref[0:1, :] = slot_of(it0, pick_t(t0, before_t).astype(jnp.int32), base, extra)
        slott_ref[1:2, :] = slot_of(it1, pick_t(t1, before_t).astype(jnp.int32), base, extra)
        g0t, g1t = softmax_pair(pick_t(t0, logits_t), pick_t(t1, logits_t))
        gatet_ref[0:1, :] = g0t
        gatet_ref[1:2, :] = g1t

    row = step * rows + lax.broadcasted_iota(jnp.int32, (rows, n_tok), 0)
    d0 = slott_ref[0:1, :] == row
    d1 = slott_ref[1:2, :] == row
    sel = jnp.where(d0 | d1, 1.0, 0.0).astype(BF16)
    g_row = jnp.sum(jnp.where(d0, gatet_ref[0:1, :], 0.0) + jnp.where(d1, gatet_ref[1:2, :], 0.0), axis=1, keepdims=True)
    sx_ref[0] = jnp.dot(sel, x_ref[...], preferred_element_type=F32).astype(BF16)
    sdy_ref[0] = (g_row * jnp.dot(sel, do_ref[...], preferred_element_type=F32)).astype(BF16)

    if share:
        @pl.when(step == n_exp - 1)
        def _():
            for copy in share_counts(cnt_ref, all_ref, send_sem, recv_sem, n_exp):
                copy.wait()
            all_ref[lax.axis_index('ep')] = cnt_ref[...]
            most_ref[...] = jnp.max(all_ref[...], axis=0)


def dispatch(tokens, grad_out, ids, w_gate, base, extra, share):
    n_tok, d_model = tokens.shape
    n_exp = w_gate.shape[1]
    rows = base + extra
    whole = lambda shape: pl.BlockSpec(shape, lambda i: (0,) * len(shape))
    block = pl.BlockSpec((1, rows, d_model), lambda i: (i, 0, 0))
    send = jax.ShapeDtypeStruct((n_exp, rows, d_model), BF16)
    out_specs = [block, block, whole((n_tok, 2)), whole((n_tok, 2))]
    out_shape = [send, send, jax.ShapeDtypeStruct((n_tok, 2), jnp.int32), jax.ShapeDtypeStruct((n_tok, 2), F32)]
    scratch = [pltpu.VMEM((2, n_tok), jnp.int32), pltpu.VMEM((2, n_tok), F32)]
    if share:
        out_specs.append(whole((8, 128)))
        out_shape.append(jax.ShapeDtypeStruct((8, 128), F32))
        scratch += [pltpu.VMEM((8, 128), F32), pltpu.VMEM((n_exp, 8, 128), F32), pltpu.SemaphoreType.DMA((n_exp,)), pltpu.SemaphoreType.DMA((n_exp,))]
    return pl.pallas_call(
        functools.partial(dispatch_kernel, base, extra, share),
        grid=(n_exp,),
        in_specs=[whole((n_tok, d_model)), whole((n_tok, d_model)), whole((n_tok, 2)), whole((2, n_tok)), whole((d_model, n_exp))],
        out_specs=out_specs,
        out_shape=out_shape,
        scratch_shapes=scratch,
        compiler_params=pltpu.CompilerParams(vmem_limit_bytes=56 * 2 ** 20, has_side_effects=share),
        cost_estimate=pl.CostEstimate(flops=4 * n_exp * rows * n_tok * d_model, bytes_accessed=4 * n_exp * rows * d_model, transcendentals=0),
        name='dispatch',
    )(tokens, grad_out, ids, ids.T, w_gate)


def gather_y_kernel(y_ref, do_ref, x_ref, ids_ref, slot_ref, gate_ref, out_ref, dl_ref, gw_ref):
    n_tile = do_ref.shape[0]
    n_exp = dl_ref.shape[1]
    col = lax.broadcasted_iota(jnp.int32, (n_tile, y_ref.shape[0]), 1)
    s0 = jnp.where(slot_ref[:, 0:1] == col, 1.0, 0.0).astype(BF16)
    s1 = jnp.where(slot_ref[:, 1:2] == col, 1.0, 0.0).astype(BF16)
    y0 = jnp.dot(s0, y_ref[...], preferred_element_type=F32)
    y1 = jnp.dot(s1, y_ref[...], preferred_element_type=F32)
    g0, g1 = gate_ref[:, 0:1], gate_ref[:, 1:2]
    out_ref[...] = (g0 * y0 + g1 * y1).astype(BF16)
    do = do_ref[...].astype(F32)
    dg0 = jnp.sum(do * y0, axis=1, keepdims=True)
    dg1 = jnp.sum(do * y1, axis=1, keepdims=True)
    mean = g0 * dg0 + g1 * dg1
    e_col = lax.broadcasted_iota(jnp.int32, (n_tile, n_exp), 1)
    dl = jnp.where(ids_ref[:, 0:1] == e_col, g0 * (dg0 - mean), 0.0) + jnp.where(ids_ref[:, 1:2] == e_col, g1 * (dg1 - mean), 0.0)
    dl = dl.astype(BF16)
    dl_ref[...] = dl

    @pl.when(pl.program_id(0) == 0)
    def _():
        gw_ref[...] = jnp.zeros_like(gw_ref)

    gw_ref[...] += lax.dot_general(x_ref[...], dl, (((0,), (0,)), ((), ())), preferred_element_type=F32)


def gather_y(y_back, grad_out, tokens, ids, slots, gates, n_exp):
    n_tok, d_model = tokens.shape
    n_slot = y_back.shape[0]
    tile = 256
    per = lambda width: pl.BlockSpec((tile, width), lambda i: (i, 0))
    return pl.pallas_call(
        gather_y_kernel,
        grid=(n_tok // tile,),
        in_specs=[pl.BlockSpec((n_slot, d_model), lambda i: (0, 0)), per(d_model), per(d_model), per(2), per(2), per(2)],
        out_specs=[per(d_model), per(n_exp), pl.BlockSpec((d_model, n_exp), lambda i: (0, 0))],
        out_shape=[jax.ShapeDtypeStruct((n_tok, d_model), BF16), jax.ShapeDtypeStruct((n_tok, n_exp), BF16), jax.ShapeDtypeStruct((d_model, n_exp), F32)],
        compiler_params=pltpu.CompilerParams(vmem_limit_bytes=56 * 2 ** 20),
        cost_estimate=pl.CostEstimate(flops=4 * n_slot * n_tok * d_model, bytes_accessed=2 * n_slot * d_model, transcendentals=0),
        name='gather_y',
    )(y_back, grad_out, tokens, ids, slots, gates)


def gather_dx_kernel(dx_ref, dl_ref, wg_ref, slot_ref, out_ref):
    col = lax.broadcasted_iota(jnp.int32, (out_ref.shape[0], dx_ref.shape[0]), 1)
    sel = jnp.where((slot_ref[:, 0:1] == col) | (slot_ref[:, 1:2] == col), 1.0, 0.0).astype(BF16)
    tot = jnp.dot(sel, dx_ref[...], preferred_element_type=F32)
    tot += lax.dot_general(dl_ref[...], wg_ref[...], (((1,), (1,)), ((), ())), preferred_element_type=F32)
    out_ref[...] = tot.astype(BF16)


def gather_dx(dx_back, d_logits, w_gate, slots):
    n_tok, n_exp = d_logits.shape
    n_slot, d_model = dx_back.shape
    tile = 256
    per = lambda width: pl.BlockSpec((tile, width), lambda i: (i, 0))
    return pl.pallas_call(
        gather_dx_kernel,
        grid=(n_tok // tile,),
        in_specs=[pl.BlockSpec((n_slot, d_model), lambda i: (0, 0)), per(n_exp), pl.BlockSpec((d_model, n_exp), lambda i: (0, 0)), per(2)],
        out_specs=per(d_model),
        out_shape=jax.ShapeDtypeStruct((n_tok, d_model), BF16),
        compiler_params=pltpu.CompilerParams(vmem_limit_bytes=56 * 2 ** 20),
        cost_estimate=pl.CostEstimate(flops=2 * n_slot * n_tok * d_model, bytes_accessed=2 * n_slot * d_model, transcendentals=0),
        name='gather_dx',
    )(dx_back, d_logits, w_gate, slots)


def gate_sum_kernel(part_ref, out_ref, all_ref, send_sem, recv_sem):
    n_dev = part_ref.shape[0]
    me = lax.axis_index('ep')
    peers = [(i, lax.rem(me + i, n_dev)) for i in range(1, n_dev)]
    first = [peer_copy(part_ref.at[d], all_ref.at[me], send_sem.at[0, i], recv_sem.at[0, i], d) for i, d in peers]
    for copy in first:
        copy.start()
    all_ref[me] = part_ref[me]
    for copy in first:
        copy.wait()
    out_ref[me] = jnp.sum(all_ref[...], axis=0)
    second = [peer_copy(out_ref.at[me], out_ref.at[me], send_sem.at[1, i], recv_sem.at[1, i], d) for i, d in peers]
    for copy in second:
        copy.start()
    for copy in second:
        copy.wait()


def gate_sum(part):
    d_model, n_exp = part.shape
    tiles = jnp.pad(part.reshape(n_exp, -1, 128), ((0, 0), (0, 2), (0, 0)))
    vmem = pl.BlockSpec(memory_space=pltpu.VMEM)
    total = pl.pallas_call(
        gate_sum_kernel,
        in_specs=[vmem],
        out_specs=vmem,
        out_shape=jax.ShapeDtypeStruct(tiles.shape, F32),
        scratch_shapes=[pltpu.VMEM(tiles.shape, F32), pltpu.SemaphoreType.DMA((2, n_exp)), pltpu.SemaphoreType.DMA((2, n_exp))],
        compiler_params=pltpu.CompilerParams(has_side_effects=True),
        name='gate_sum',
    )(tiles)
    return total[:, :6].reshape(d_model, n_exp)


def exchange(value):
    return lax.all_to_all(value, 'ep', 0, 0, tiled=True)


def expert_fwd(rows, w_one, w_two):
    a_pre = jnp.dot(rows, w_one, preferred_element_type=F32)
    hidden, gelu_vjp = jax.vjp(jax.nn.gelu, a_pre)
    hid_b = hidden.astype(BF16)
    y_rows = jnp.dot(hid_b, w_two, preferred_element_type=F32).astype(BF16)
    return hid_b, gelu_vjp, y_rows


def expert_bwd(dy_rows, gelu_vjp, w_one, w_two):
    d_hid = jnp.einsum('rm,hm->rh', dy_rows, w_two, preferred_element_type=F32)
    d_pre = gelu_vjp(d_hid)[0].astype(BF16)
    return d_pre, jnp.einsum('rh,mh->rm', d_pre, w_one, preferred_element_type=F32).astype(BF16)


def weight_grads(rows, hid_b, dy_rows, d_pre):
    g_two = jnp.einsum('rh,rm->hm', hid_b, dy_rows, preferred_element_type=F32)
    g_one = jnp.einsum('rm,rh->mh', rows, d_pre, preferred_element_type=F32)
    return g_one, g_two


def padded_path(tokens, grad_out, ids, w_gate, w_one, w_two, mine, *sent):
    n_exp = w_gate.shape[1]
    n_row, d_model = n_exp * FULL, tokens.shape[1]
    send_x, send_dy, slots, gates = dispatch(tokens, grad_out, ids, w_gate, FULL, 0, False)
    x_rows = exchange(send_x).reshape(n_row, d_model)
    dy_rows = exchange(send_dy).reshape(n_row, d_model)
    hid_b, gelu_vjp, y_rows = expert_fwd(x_rows, w_one, w_two)
    y_back = exchange(y_rows.reshape(n_exp, FULL, d_model)).reshape(n_row, d_model)
    d_pre, dx_rows = expert_bwd(dy_rows, gelu_vjp, w_one, w_two)
    dx_back = exchange(dx_rows.reshape(n_exp, FULL, d_model)).reshape(n_row, d_model)
    g_one, g_two = weight_grads(x_rows, hid_b, dy_rows, d_pre)
    y_out, d_logits, gw_part = gather_y(y_back, grad_out, tokens, ids, slots, gates, n_exp)
    grad_x = gather_dx(dx_back, d_logits, w_gate, slots)
    return y_out, grad_x, g_one, g_two, gate_sum(gw_part)


HID_TILE = 512
CHUNK = 4
C_IN = 0.044715
C_OUT = 0.7978845608028654


def xor_peer(me, i):
    return sum(lax.rem(lax.div(me, 1 << b) + lax.div(i, 1 << b), 2) * (1 << b) for b in range(4))


def gelu_parts(a):
    sq = a * a
    t = jnp.tanh(C_OUT * a * (1.0 + C_IN * sq))
    cdf = 0.5 * (1.0 + t)
    return sq, t, cdf


def middle_kernel(mine_ref, sx_ref, sdy_ref, w1_ref, w2_ref, yb_ref, dxb_ref, g1_ref, g2_ref,
                  w1v, w2v, h1v, h2v, a1, a2, xb, xe, db, de, xo, do, yb_s, ye_s, acc, ssem, rsem, wssem, wrsem, lsem):
    n_dev = sx_ref.shape[0]
    n_hid = w1v.shape[1]
    n_tile = n_hid // HID_TILE
    me = lax.axis_index('ep')
    partner = me + 1 - 2 * lax.rem(me, 2)
    size = (BASE, EXTRA)
    start = (0, BASE)
    land = ((xb, xe), (db, de))
    leave = ((yb_s, ye_s), (db, xe))
    sent = (sx_ref, sdy_ref)
    home = (yb_ref, dxb_ref)

    def rows_of(ref, kind, i):
        return ref.at[pl.ds(pl.multiple_of(i * size[kind], 16), size[kind])]

    def ends(ex, kind, i):
        if ex < 2:
            return sent[ex].at[xor_peer(me, i), pl.ds(start[kind], size[kind])], rows_of(land[ex][kind], kind, i)
        there = home[ex - 2].at[pl.ds(pl.multiple_of(me * (BASE + EXTRA) + start[kind], 16), size[kind])]
        return rows_of(leave[ex - 2][kind], kind, i), there

    def remote(ex, kind, i):
        src, dst = ends(ex, kind, i)
        return peer_copy(src, dst, ssem.at[ex, kind, i], rsem.at[ex, kind, i], xor_peer(me, i))

    def local(ex, kind):
        src, dst = ends(ex, kind, 0)
        return pltpu.make_async_copy(src, dst, rsem.at[ex, kind, 0])

    def send_all(ex, kind):
        local(ex, kind).start()

        def body(i, _):
            remote(ex, kind, i).start()
            return 0

        lax.fori_loop(1, n_dev, body, 0)

    def send_chunk(ex, kind, c):
        @pl.when(c == 0)
        def _():
            local(ex, kind).start()

        @pl.when(c > 0)
        def _():
            remote(ex, kind, c * CHUNK).start()

        for j in range(1, CHUNK):
            remote(ex, kind, c * CHUNK + j).start()

    def landed(ex, kind, i):
        remote(ex, kind, i).wait_recv()

    def get_chunk(ex, kind, c):
        for j in range(CHUNK):
            landed(ex, kind, c * CHUNK + j)

    w1_in = pltpu.make_async_copy(w1_ref, w1v, lsem.at[0])
    w2_in = pltpu.make_async_copy(w2_ref, w2v, lsem.at[1])
    w1_in.start()
    w2_in.start()
    send_all(0, 0)
    send_all(0, 1)
    swaps = [peer_copy(src, dst, wssem.at[k], wrsem.at[k], partner) for k, (src, dst) in enumerate([(w1_ref, h1v), (w2_ref, h2v), (xe, xo), (de, do)])]
    swaps[0].start()
    swaps[1].start()

    def zero(k, _):
        a1[pl.ds(pl.multiple_of(k * 64, 64), 64)] = jnp.zeros((64, n_hid), F32)
        a2[pl.ds(pl.multiple_of(k * 256, 256), 256)] = jnp.zeros((256, a2.shape[1]), F32)
        return 0

    lax.fori_loop(0, n_tile * 2, zero, 0)
    w1_in.wait()
    w2_in.wait()

    def forward(kind, u1, u2, c):
        n_row = CHUNK * size[kind]
        here = pl.ds(pl.multiple_of(c * n_row, 64), n_row)
        x_buf, y_buf = land[0][kind], leave[0][kind]
        acc[pl.ds(0, n_row)] = jnp.zeros((n_row, acc.shape[1]), F32)

        def tile(k, _):
            cols = pl.ds(pl.multiple_of(k * HID_TILE, HID_TILE), HID_TILE)
            a = jnp.dot(x_buf[here], u1[:, cols], preferred_element_type=F32)
            hid = (a * gelu_parts(a)[2]).astype(BF16)
            acc[pl.ds(0, n_row)] += jnp.dot(hid, u2[cols, :], preferred_element_type=F32)
            return 0

        lax.fori_loop(0, n_tile, tile, 0)
        y_buf[here] = acc[pl.ds(0, n_row)].astype(BF16)

    def backward(n_row, x_buf, d_buf, u1, u2, mask, dx_buf, c):
        here = pl.ds(pl.multiple_of(c * n_row, 64), n_row)
        want = dx_buf is not None
        if want:
            acc[pl.ds(0, n_row)] = jnp.zeros((n_row, acc.shape[1]), F32)

        def tile(k, _):
            cols = pl.ds(pl.multiple_of(k * HID_TILE, HID_TILE), HID_TILE)
            x, dy = x_buf[here], d_buf[here]
            a = jnp.dot(x, u1[:, cols], preferred_element_type=F32)
            sq, t, cdf = gelu_parts(a)
            hid = (a * cdf).astype(BF16)
            slope = cdf + (0.5 * C_OUT) * a * (1.0 - t * t) * (1.0 + (3.0 * C_IN) * sq)
            dh = lax.dot_general(dy, u2[cols, :], (((1,), (1,)), ((), ())), preferred_element_type=F32)
            da = (dh * slope).astype(BF16)
            if want:
                acc[pl.ds(0, n_row)] += lax.dot_general(da, u1[:, cols], (((1,), (1,)), ((), ())), preferred_element_type=F32)
            if mask is not None:
                x = (x.astype(F32) * mask).astype(BF16)
                dy = (dy.astype(F32) * mask).astype(BF16)
            a2[cols, :] += lax.dot_general(hid, dy, (((0,), (0,)), ((), ())), preferred_element_type=F32)
            a1[:, cols] += lax.dot_general(x, da, (((0,), (0,)), ((), ())), preferred_element_type=F32)
            return 0

        lax.fori_loop(0, n_tile, tile, 0)
        if want:
            dx_buf[here] = acc[pl.ds(0, n_row)].astype(BF16)

    n_chunk = n_dev // CHUNK

    def fwd_base(c, _):
        get_chunk(0, 0, c)

        @pl.when(c == 1)
        def _():
            send_all(1, 0)

        @pl.when(c == 2)
        def _():
            send_all(1, 1)

        forward(0, w1v, w2v, c)
        send_chunk(2, 0, c)
        return 0

    lax.fori_loop(0, n_chunk, fwd_base, 0)
    swaps[0].wait_recv()
    swaps[1].wait_recv()
    mine = mine_ref[0].astype(F32)

    def choose(k, _):
        for own, hot, n_row in ((w1v, h1v, 64), (w2v, h2v, 256)):
            here = pl.ds(pl.multiple_of(k * n_row, n_row), n_row)
            hot[here] = (own[here].astype(F32) * mine + hot[here].astype(F32) * (1.0 - mine)).astype(BF16)
        return 0

    lax.fori_loop(0, n_tile * 2, choose, 0)

    def fwd_extra(c, _):
        get_chunk(0, 1, c)
        forward(1, h1v, h2v, c)
        send_chunk(2, 1, c)
        return 0

    lax.fori_loop(0, n_chunk, fwd_extra, 0)
    swaps[2].start()

    def bwd_base(c, _):
        get_chunk(1, 0, c)
        backward(CHUNK * BASE, xb, db, w1v, w2v, None, db, c)
        send_chunk(3, 0, c)
        return 0

    lax.fori_loop(0, n_chunk, bwd_base, 0)
    swaps[2].wait_send()

    def get_extra(c, _):
        get_chunk(1, 1, c)
        return 0

    lax.fori_loop(0, n_chunk, get_extra, 0)
    swaps[3].start()

    def bwd_extra(c, _):
        backward(CHUNK * EXTRA, xe, de, h1v, h2v, mine, xe, c)
        send_chunk(3, 1, c)
        return 0

    lax.fori_loop(0, n_chunk, bwd_extra, 0)
    swaps[2].wait_recv()
    swaps[3].wait_recv()

    def bwd_other(c, _):
        backward(2 * CHUNK * EXTRA, xo, do, w1v, w2v, mine, None, c)
        return 0

    lax.fori_loop(0, n_chunk // 2, bwd_other, 0)
    flush = [pltpu.make_async_copy(a1, g1_ref, lsem.at[0]), pltpu.make_async_copy(a2, g2_ref, lsem.at[1])]
    for copy in flush:
        copy.start()
    swaps[0].wait_send()
    swaps[1].wait_send()
    swaps[3].wait_send()

    def finish(i, _):
        for kind in range(2):
            for ex in range(4):
                @pl.when(i > 0)
                def _():
                    remote(ex, kind, i).wait_send()
            for ex in range(2, 4):
                landed(ex, kind, i)
        return 0

    lax.fori_loop(0, n_dev, finish, 0)
    for copy in flush:
        copy.wait()


def middle(mine, send_x, send_dy, w_one, w_two):
    n_dev, rows, d_model = send_x.shape
    n_hid = w_one.shape[1]
    hbm = pl.BlockSpec(memory_space=pl.ANY)
    back = jax.ShapeDtypeStruct((n_dev * rows, d_model), BF16)
    wide = lambda n_row, kind: pltpu.VMEM((n_row, d_model), kind)
    n_base, n_extra = n_dev * BASE, n_dev * EXTRA
    dma = pltpu.SemaphoreType.DMA
    return pl.pallas_call(
        middle_kernel,
        in_specs=[pl.BlockSpec(memory_space=pltpu.SMEM)] + [hbm] * 4,
        out_specs=[hbm] * 4,
        out_shape=[back, back, jax.ShapeDtypeStruct((d_model, n_hid), F32), jax.ShapeDtypeStruct((n_hid, d_model), F32)],
        scratch_shapes=[
            pltpu.VMEM((d_model, n_hid), BF16), wide(n_hid, BF16), pltpu.VMEM((d_model, n_hid), BF16), wide(n_hid, BF16),
            pltpu.VMEM((d_model, n_hid), F32), wide(n_hid, F32),
            wide(n_base, BF16), wide(n_extra, BF16), wide(n_base, BF16), wide(n_extra, BF16), wide(n_extra, BF16), wide(n_extra, BF16),
            wide(n_base, BF16), wide(n_extra, BF16), wide(CHUNK * BASE, F32),
            dma((4, 2, n_dev)), dma((4, 2, n_dev)), dma((4,)), dma((4,)), dma((2,)),
        ],
        compiler_params=pltpu.CompilerParams(vmem_limit_bytes=67043328, has_side_effects=True),
        cost_estimate=pl.CostEstimate(flops=14 * n_dev * rows * d_model * n_hid, bytes_accessed=4 * n_hid * d_model * 6, transcendentals=0),
        name='middle',
    )(mine, send_x, send_dy, w_one, w_two)


def shared_path(tokens, grad_out, ids, w_gate, w_one, w_two, mine, send_x, send_dy, slots, gates):
    mine = mine.astype(jnp.int32).reshape(1)
    y_back, dx_back, g_one, g_two = middle(mine, send_x, send_dy, w_one, w_two)
    y_out, d_logits, gw_part = gather_y(y_back, grad_out, tokens, ids, slots, gates, w_gate.shape[1])
    grad_x = gather_dx(dx_back, d_logits, w_gate, slots)
    return y_out, grad_x, g_one, g_two, gate_sum(gw_part)


def local_block(tokens, grad_out, expert_ids, w_gate, w_in, w_out):
    n_exp = w_gate.shape[1]
    *sent, most = dispatch(tokens, grad_out, expert_ids, w_gate, BASE, EXTRA, True)
    over = most[0, :n_exp] > BASE
    mine = over[lax.axis_index('ep')]
    both = jnp.any(over.reshape(n_exp // 2, 2).all(axis=1))
    args = (tokens, grad_out, expert_ids, w_gate, w_in[0], w_out[0], mine, *sent)
    y_out, grad_x, g_one, g_two, g_gate = lax.cond(both, padded_path, shared_path, *args)
    return y_out, grad_x, g_one[None], g_two[None], g_gate


def solution(mesh):
    return jax.shard_map(local_block, mesh=mesh, in_specs=(P('ep'), P('ep'), P('ep'), P(), P('ep'), P('ep')), out_specs=(P('ep'), P('ep'), P('ep'), P('ep'), P()), check_vma=False)
```
